512 devices in a mesh: seqa: 16 (over z_lo, core), seqb: 8 (over x, z_hi), dp: 4 (over y).
Axes of the slice: x: 4, y: 4, z: 16 (z_hi: 2, z_lo: 8; z = z_hi * 8 + z_lo), core: 2. Of those that a mesh axis runs over, the one named last changes fastest.
Arguments:
- queries: bfloat16 [16384, 128, 64], P(('dp', 'seqa', 'seqb')), parts along dimension 0, may hold values from -6 to 6
- keys: bfloat16 [16384, 128, 64], P(('dp', 'seqa', 'seqb')), parts along dimension 0, may hold values from -6 to 6
- values: bfloat16 [16384, 128, 64], P(('dp', 'seqa', 'seqb')), parts along dimension 0, may hold values from -6 to 6
- doc_bounds: int32 [36], P('dp'), parts along dimension 0, may hold values from 0 to 4096, as said below
- q_gain: float32 [64], replicated, may hold values from 0.25 to 1.75
- k_gain: float32 [64], replicated, may hold values from 0.25 to 1.75
Outputs:
- attended: bfloat16 [16384, 128, 64], P(('dp', 'seqa', 'seqb')), parts along dimension 0
The draws below stay inside these ranges and needn't reach their ends.
There are 4 independent parts, one for each index of `dp`. The reference program is written for one: setup_inputs(seed, part) draws one part's arguments, and reference() takes and returns one part's arrays. A program takes and returns all parts, laid end to end along the dimension named above; an argument that names none is the same for every part. Nothing has to cross between parts.
Inputs may be any that keep to these rules, and one draw needn't show every extreme that they name: doc_bounds[0] is 0, doc_bounds[8] is 4096, and the entries rise strictly.
All inputs are finite; a program needn't handle non-finite values.
Results may differ from the reference program's by a relative error of at most 0.0015.
Values may be sent and summed in bfloat16 or wider, within the bound.
A program may use at most 64 MiB of HBM per device.

```python
import jax
import jax.numpy as jnp
from jax import lax

HD = 64
DOCS = 8
SEQ = 4096
HEADS = 128


def draw_doc_bounds(key, part):
    shuffled = jax.random.permutation(key, SEQ - 1).astype(jnp.int32) + 1
    cuts = jnp.sort(shuffled[:DOCS - 1])
    return jnp.concatenate([jnp.zeros((1,), jnp.int32), cuts, jnp.full((1,), SEQ, jnp.int32)]).astype(jnp.int32)


def level_of(stream_key, shape, cuts, least, top_value):
    def one(dim, parts):
        heights = jax.random.uniform(jax.random.fold_in(jax.random.fold_in(stream_key, 6), dim), (parts,), jnp.float32, least / len(cuts), top_value / len(cuts))
        return jnp.repeat(jnp.exp(heights), shape[dim] // parts).reshape((-1,) + (1,) * (len(shape) - dim - 1))

    level = one(*cuts[0])
    for cut in cuts[1:]:
        level = level * one(*cut)
    return level


def normal_values(stream_key, dims, scale, bound, shards=(), kind=jnp.bfloat16):
    values = scale * jax.random.normal(stream_key, dims, jnp.float32)
    if shards:
        values = values * level_of(stream_key, dims, shards, -0.22, 0.18)
    return jnp.clip(values, -bound, bound).astype(kind)


def setup_inputs(seed: int = 0, part: int = 0) -> dict:
    streams_of = jax.random.split(jax.random.key(seed), 7)
    part_keys = jax.random.split(jax.random.fold_in(streams_of[6], part), 7)
    queries = normal_values(part_keys[0], (SEQ, HEADS, HD), 1.0, 6.0, ((0, 128),))
    keys = normal_values(part_keys[1], (SEQ, HEADS, HD), 1.0, 6.0, ((0, 128),))
    values = normal_values(part_keys[2], (SEQ, HEADS, HD), 1.0, 6.0, ((0, 128),))
    doc_bounds = draw_doc_bounds(jax.random.fold_in(jax.random.fold_in(streams_of[6], part), 71), part)
    q_gain = jnp.clip(1.0 + 0.15 * jax.random.normal(streams_of[4], (HD,), jnp.float32), 0.25, 1.75)
    k_gain = jnp.clip(1.0 + 0.15 * jax.random.normal(streams_of[5], (HD,), jnp.float32), 0.25, 1.75)
    return {"queries": queries, "keys": keys, "values": values, "doc_bounds": doc_bounds, "q_gain": q_gain, "k_gain": k_gain}


def prepare(block, gain, positions):
    values32 = block.astype(jnp.float32)
    scale = lax.rsqrt(lax.optimization_barrier(jnp.mean(values32 * values32, axis=-1, keepdims=True)) + 1e-06)
    normed = values32 * scale * gain
    half = normed.shape[-1] // 2
    freq = jnp.exp(-jnp.log(10000.0) * jnp.arange(half, dtype=jnp.float32) * 2.0 / normed.shape[-1])
    angle = positions.astype(jnp.float32)[:, None] * freq[None, :]
    first = normed[:, :half]
    second = normed[:, half:]
    cosine = jnp.cos(angle)
    sine = jnp.sin(angle)
    rotated = jnp.concatenate([first * cosine - second * sine, first * sine + second * cosine], axis=-1)
    return rotated.astype(jnp.bfloat16)

def reference(queries, keys, values, doc_bounds, q_gain, k_gain):
    length = queries.shape[0]
    width = queries.shape[2]
    places = jnp.arange(length, dtype=jnp.int32)
    doc = lax.optimization_barrier(jnp.sum((places[:, None] >= doc_bounds[None, 1:DOCS]).astype(jnp.int32), axis=1)).astype(jnp.int32)
    positions = places - doc_bounds[doc]
    allowed = (doc[:, None] == doc[None, :]) & (places[None, :] <= places[:, None])

    def one_head(items):
        query_head, key_head, value_head = items
        qr = prepare(query_head, q_gain, positions)
        kr = prepare(key_head, k_gain, positions)
        scores = jnp.dot(qr, kr.T, preferred_element_type=jnp.float32) / jnp.sqrt(jnp.float32(width))
        scores = jnp.where(allowed, scores, jnp.float32(-1e+30))
        top = lax.optimization_barrier(jnp.max(scores, axis=1, keepdims=True))
        expo = jnp.where(allowed, jnp.exp(scores - top), jnp.float32(0.0))
        weights = (expo / lax.optimization_barrier(jnp.sum(expo, axis=1, keepdims=True))).astype(jnp.bfloat16)
        return jnp.dot(weights, value_head, preferred_element_type=jnp.float32).astype(jnp.bfloat16)
    outputs = lax.map(one_head, (jnp.transpose(queries, (1, 0, 2)), jnp.transpose(keys, (1, 0, 2)), jnp.transpose(values, (1, 0, 2))))
    return jnp.transpose(outputs, (1, 0, 2))
```

```python
import functools
import math

import jax
import jax.numpy as jnp
import numpy as np
from jax import lax
from jax.experimental import pallas as pl
from jax.experimental.pallas import tpu as pltpu
from jax.sharding import PartitionSpec as P

MESH = pl.DeviceIdType.MESH
DOCS = 8
TOK, HEADS, WIDTH = 32, 128, 64
N, NB = 128, 8
HALF = TOK // 2
SUB = HALF // 2
TILES = 8
PER = N // TILES
SCALE = math.log2(math.e) / math.sqrt(WIDTH)
LOG_BASE = np.float32(-np.log(np.float32(10000.0)))
FREQS = [
    float(np.float32(np.exp(np.float64(np.float32(LOG_BASE * np.float32(i)) * 2.0 / WIDTH))))
    for i in range(WIDTH // 2)
]


def cos_sin(angle):
    turns = jnp.floor(angle * 0.6366197723675814 + 0.5)
    r = angle - turns * 1.5703125
    r = r - turns * 4.837512969970703125e-4
    r = r - turns * 7.54978995489188216e-8
    z = r * r
    s = ((-1.9515295891e-4 * z + 8.3321608736e-3) * z - 1.6666654611e-1) * z * r + r
    c = ((2.443315711809948e-5 * z - 1.388731625493765e-3) * z + 4.166664568298827e-2) * z * z
    c = c - 0.5 * z + 1.0
    quarter = turns.astype(jnp.int32)
    odd = (quarter & 1) == 1
    cosine = jnp.where(odd, s, c)
    sine = jnp.where(odd, c, s)
    cosine = jnp.where(((quarter + 1) & 2) == 2, -cosine, cosine)
    sine = jnp.where((quarter & 2) == 2, -sine, sine)
    return cosine, sine


def start_of(place, doc):
    start = jnp.zeros_like(place)
    for d in range(1, DOCS):
        start = jnp.where(place >= doc[d], doc[d], start)
    return start


def coords(p):
    return {"seqa": p // NB, "seqb": lax.rem(p, NB)}


def peer_of(me, m):
    zl, c, x, zh = me // 16, lax.rem(me // 8, 2), lax.rem(me // 2, 4), lax.rem(me, 2)
    k, r = lax.rem(m, 16), m // 16
    dz = jnp.where(lax.rem(k, 2) == 0, 16 - k // 2, (k + 1) // 2)
    z = lax.rem(zh * 8 + zl + dz, 16)
    x = lax.rem(x + r // 2, 4)
    c = lax.rem(c + r, 2)
    return ((lax.rem(z, 8) * 2 + c) * 4 + x) * 2 + z // 8


def kernel(
    q_hbm, k_hbm, v_hbm, doc_hbm, qg_hbm, kg_hbm, out_ref,
    qb, kb, vb, doc, gains, stage, send_a, send_b, recv_a, recv_b, vt, probs, kpos, wq,
    back, gathered, rows_out,
    in_sem, send_sem, ra_sem, rb_sem, back_send, back_recv,
):
    me = lax.axis_index("seqa") * NB + lax.axis_index("seqb")
    barrier = pltpu.get_barrier_semaphore()

    def greet(m, carry):
        p = lax.rem(me + m, N)
        pl.semaphore_signal(barrier, inc=1, device_id=coords(p), device_id_type=MESH)
        return carry

    lax.fori_loop(1, N, greet, 0)
    loads = [
        pltpu.make_async_copy(src, dst, in_sem.at[i])
        for i, (src, dst) in enumerate(
            (
                (doc_hbm, doc), (qg_hbm, gains.at[0]), (kg_hbm, gains.at[1]),
                (q_hbm, qb), (k_hbm, kb), (v_hbm, vb),
            )
        )
    ]
    for load in loads:
        load.start()
    for load in loads:
        load.wait()

    row = lax.broadcasted_iota(jnp.int32, (WIDTH // 2, HEADS), 0)
    freq = jnp.zeros((WIDTH // 2, HEADS), jnp.float32)
    for i, f in enumerate(FREQS):
        freq = jnp.where(row == i, jnp.float32(f), freq)
    gq, gk = (
        jnp.transpose(jnp.broadcast_to(gains[i], (HEADS, WIDTH)), (1, 0)) for i in range(2)
    )

    def prepared(x, gain, cosine, sine):
        x = x.astype(jnp.float32)
        mean = jnp.sum(x * x, axis=0, keepdims=True) * (1.0 / WIDTH)
        x = x * lax.rsqrt(mean + 1e-06) * gain
        a, b = x[: WIDTH // 2], x[WIDTH // 2 :]
        return a * cosine - b * sine, a * sine + b * cosine

    def pair_rows(r, carry):
        parts_q, parts_k, parts_v = [], [], []
        for t in (r, r + HALF):
            place = me * TOK + t
            pos = (place - start_of(place, doc)).astype(jnp.float32)
            cosine, sine = cos_sin(pos * freq)
            parts_q.extend(prepared(qb[t], gq, cosine, sine))
            parts_k.extend(prepared(kb[t], gk, cosine, sine))
            parts_v.append(vb[t].astype(jnp.float32))
        for at, parts in ((0, parts_k), (HALF, parts_v), (2 * HALF, parts_q)):
            block = jnp.transpose(jnp.concatenate(parts, axis=0), (1, 0))
            stage[pl.ds(at + r, HEADS, stride=3 * HALF), :] = block
        return carry

    lax.fori_loop(0, HALF, pair_rows, 0)

    def pack(h, carry):
        rows = stage[pl.ds(pl.multiple_of(h * 8 * 3 * HALF, 8), 8 * 3 * HALF), :]
        rows = rows.reshape(8, 3 * HALF, 2 * WIDTH)
        send_a[pl.ds(h * 8, 8)] = rows[:, : 2 * HALF + SUB].astype(jnp.bfloat16)
        send_b[pl.ds(h * 8, 8)] = rows[:, 2 * HALF + SUB :].astype(jnp.bfloat16)
        return carry

    lax.fori_loop(0, HEADS // 8, pack, 0)

    pl.semaphore_wait(barrier, N - 1)

    my_tile = me // PER

    def post_a(m, carry):
        p = peer_of(me, m)
        pltpu.make_async_remote_copy(
            src_ref=send_a.at[p], dst_ref=recv_a.at[me], send_sem=send_sem.at[0],
            recv_sem=ra_sem.at[my_tile], device_id=coords(p), device_id_type=MESH,
        ).start()
        return carry

    def post_b(m, carry):
        p = peer_of(me, m)
        pltpu.make_async_remote_copy(
            src_ref=send_b.at[p], dst_ref=recv_b.at[me], send_sem=send_sem.at[1],
            recv_sem=rb_sem.at[my_tile], device_id=coords(p), device_id_type=MESH,
        ).start()
        return carry

    lax.fori_loop(1, N, post_a, 0)
    lax.fori_loop(1, N, post_b, 0)
    own_a = pltpu.make_async_copy(send_a.at[me], recv_a.at[me], ra_sem.at[my_tile])
    own_b = pltpu.make_async_copy(send_b.at[me], recv_b.at[me], rb_sem.at[my_tile])
    own_a.start()
    own_b.start()

    key_row = lax.broadcasted_iota(jnp.int32, (PER * HALF, 2 * WIDTH), 0)
    kpos[...] = lax.rem(key_row, HALF) + (key_row // HALF) * TOK

    def arrived(ref, sem, j):
        part = ref.at[pl.ds(j * PER, PER)]
        pltpu.make_async_copy(part, part, sem.at[j]).wait()

    for j in range(TILES):
        arrived(recv_a, ra_sem, j)
    for j in range(TILES):
        v = recv_a[j * PER : (j + 1) * PER, HALF : 2 * HALF, :].reshape(PER * HALF, 2 * WIDTH)
        v = jnp.transpose(v.astype(jnp.float32), (1, 0)).astype(jnp.bfloat16)
        vt[j, :, : PER * HALF] = v[:WIDTH]
        vt[j, :, PER * HALF :] = v[WIDTH:]

    low = lax.broadcasted_iota(jnp.int32, (PER * SUB, 2 * WIDTH), 1) < WIDTH
    queries = 2 * PER * SUB
    span = PER * TOK

    def tile(i, g):
        if g == 0:
            x = recv_a[i * PER : (i + 1) * PER, 2 * HALF :, :]
        else:
            x = recv_b[i * PER : (i + 1) * PER]
        x = x.astype(jnp.float32).reshape(PER * SUB, 2 * WIDTH)
        turned = pltpu.roll(x, WIDTH, 1)
        zero = jnp.zeros_like(x)
        wq[0, : PER * SUB] = jnp.where(low, x, zero).astype(jnp.bfloat16)
        wq[0, PER * SUB :] = jnp.where(low, turned, zero).astype(jnp.bfloat16)
        wq[1, : PER * SUB] = jnp.where(low, zero, turned).astype(jnp.bfloat16)
        wq[1, PER * SUB :] = jnp.where(low, zero, x).astype(jnp.bfloat16)
        lane = lax.broadcasted_iota(jnp.int32, (1, queries), 1)
        within = lax.rem(lane, PER * SUB)
        place = (
            i * span + (within // SUB) * TOK + lax.rem(within, SUB) + g * SUB
            + jnp.where(lane >= PER * SUB, HALF, 0)
        )
        start = start_of(place, doc)
        total = jnp.zeros((8, queries), jnp.float32)
        for j in range(i + 1):
            keys = recv_a[j * PER : (j + 1) * PER, :HALF, :].reshape(PER * HALF, 2 * WIDTH)
            for half in range(2):
                scores = lax.dot_general(
                    keys, wq[half], (((1,), (1,)), ((), ())), preferred_element_type=jnp.float32
                )
                at = jnp.concatenate([kpos[...], kpos[...]], axis=1)
                base = j * span + half * HALF
                allowed = at >= start - base
                if j == i:
                    allowed = allowed & (at <= place - base)
                p = jnp.where(allowed, jnp.exp2(scores * SCALE), 0.0)
                probs[j, half * PER * HALF : (half + 1) * PER * HALF] = p
                total = total + jnp.sum(p.reshape(PER * HALF // 8, 8, queries), axis=0)
        inverse = 1.0 / jnp.sum(total, axis=0, keepdims=True)
        out = jnp.zeros((WIDTH, queries), jnp.float32)
        for j in range(i + 1):
            weights = (probs[j] * inverse).astype(jnp.bfloat16)
            out = out + jnp.dot(vt[j], weights, preferred_element_type=jnp.float32)
        out = jnp.concatenate([out[:, : PER * SUB], out[:, PER * SUB :]], axis=0)
        out = jnp.transpose(out, (1, 0)).reshape(PER, SUB, 2 * WIDTH)
        back[g, i * PER : (i + 1) * PER] = out.astype(jnp.bfloat16)

    def go_home(i, g):
        def one(s, carry):
            p = i * PER + s

            @pl.when(p != me)
            def _():
                pltpu.make_async_remote_copy(
                    src_ref=back.at[g, p], dst_ref=gathered.at[g, me], send_sem=back_send.at[g],
                    recv_sem=back_recv.at[g], device_id=coords(p), device_id_type=MESH,
                ).start()

            return carry

        lax.fori_loop(0, PER, one, 0)

    for g in range(2):
        if g == 1:
            for j in range(TILES):
                arrived(recv_b, rb_sem, j)

        def step(t, carry):
            i = lax.rem(my_tile + t, TILES)
            lax.switch(i, [functools.partial(tile, k, g) for k in range(TILES)])
            go_home(i, g)
            return carry

        lax.fori_loop(0, TILES, step, 0)

    def others(ref):
        part = ref.at[pl.ds(1, N - 1)]
        return part, part

    for g in range(2):
        gathered[g, me] = back[g, me]
        pltpu.make_async_copy(*others(gathered.at[g]), back_recv.at[g]).wait()
        rows_out[...] = gathered[g].astype(jnp.float32).reshape(HEADS * SUB, 2 * WIDTH)
        for r in range(SUB):
            block = jnp.transpose(rows_out[pl.ds(r, HEADS, stride=SUB), :], (1, 0))
            block = block.astype(jnp.bfloat16)
            out_ref[g * SUB + r] = block[:WIDTH]
            out_ref[g * SUB + r + HALF] = block[WIDTH:]
    pltpu.make_async_copy(*others(send_a), send_sem.at[0]).wait()
    pltpu.make_async_copy(*others(send_b), send_sem.at[1]).wait()
    for g in range(2):
        pltpu.make_async_copy(*others(back.at[g]), back_send.at[g]).wait()


def attention(queries, keys, values, doc_bounds, q_gain, k_gain):
    tok, heads, width = queries.shape
    assert (tok, heads, width) == (TOK, HEADS, WIDTH)
    queries, keys, values = (jnp.transpose(a, (0, 2, 1)) for a in (queries, keys, values))
    block = pltpu.VMEM((TOK, WIDTH, HEADS), jnp.bfloat16)
    bf16, f32 = jnp.bfloat16, jnp.float32
    dma = pltpu.SemaphoreType.DMA
    out = pl.pallas_call(
        kernel,
        out_shape=jax.ShapeDtypeStruct((TOK, WIDTH, HEADS), bf16),
        in_specs=[pl.BlockSpec(memory_space=pl.ANY)] * 6,
        out_specs=pl.BlockSpec(memory_space=pltpu.VMEM),
        scratch_shapes=[
            block, block, block,
            pltpu.SMEM(doc_bounds.shape, jnp.int32),
            pltpu.VMEM((2, 1, WIDTH), f32),
            pltpu.VMEM((HEADS * 3 * HALF, 2 * WIDTH), f32),
            pltpu.VMEM((N, 2 * HALF + SUB, 2 * WIDTH), bf16),
            pltpu.VMEM((N, SUB, 2 * WIDTH), bf16),
            pltpu.VMEM((N, 2 * HALF + SUB, 2 * WIDTH), bf16),
            pltpu.VMEM((N, SUB, 2 * WIDTH), bf16),
            pltpu.VMEM((TILES, WIDTH, 2 * PER * HALF), bf16),
            pltpu.VMEM((TILES, 2 * PER * HALF, 2 * PER * SUB), f32),
            pltpu.VMEM((PER * HALF, 2 * WIDTH), jnp.int32),
            pltpu.VMEM((2, 2 * PER * SUB, 2 * WIDTH), bf16),
            pltpu.VMEM((2, N, SUB, 2 * WIDTH), bf16),
            pltpu.VMEM((2, N, SUB, 2 * WIDTH), bf16),
            pltpu.VMEM((HEADS * SUB, 2 * WIDTH), f32),
            dma((6,)), dma((2,)), dma((TILES,)), dma((TILES,)), dma((2,)), dma((2,)),
        ],
        compiler_params=pltpu.CompilerParams(
            collective_id=0, has_side_effects=True, vmem_limit_bytes=60 << 20
        ),
    )(queries, keys, values, doc_bounds, q_gain.reshape(1, WIDTH), k_gain.reshape(1, WIDTH))
    return jnp.transpose(out, (0, 2, 1))


def solution(mesh):
    assert mesh.shape["seqa"] * mesh.shape["seqb"] == N and mesh.shape["seqb"] == NB
    rows = P(("dp", "seqa", "seqb"), None, None)
    return jax.shard_map(
        attention,
        mesh=mesh,
        in_specs=(rows, rows, rows, P("dp"), P(), P()),
        out_specs=rows,
        check_vma=False,
    )
```

```python
import functools
import math

import jax
import jax.numpy as jnp
import numpy as np
from jax import lax
from jax.experimental import pallas as pl
from jax.experimental.pallas import tpu as pltpu
from jax.sharding import PartitionSpec as P

MESH = pl.DeviceIdType.MESH
DOCS = 8
TOK, HEADS, WIDTH = 32, 128, 64
N, NB = 128, 8
HALF = TOK // 2
SUB = HALF // 2
TILES = 8
PER = N // TILES
SCALE = math.log2(math.e) / math.sqrt(WIDTH)
LOG_BASE = np.float32(-np.log(np.float32(10000.0)))
FREQS = [
    float(np.float32(np.exp(np.float64(np.float32(LOG_BASE * np.float32(i)) * 2.0 / WIDTH))))
    for i in range(WIDTH // 2)
]


def cos_sin(angle):
    turns = jnp.floor(angle * 0.6366197723675814 + 0.5)
    r = angle - turns * 1.5703125
    r = r - turns * 4.837512969970703125e-4
    r = r - turns * 7.54978995489188216e-8
    z = r * r
    s = ((-1.9515295891e-4 * z + 8.3321608736e-3) * z - 1.6666654611e-1) * z * r + r
    c = ((2.443315711809948e-5 * z - 1.388731625493765e-3) * z + 4.166664568298827e-2) * z * z
    c = c - 0.5 * z + 1.0
    quarter = turns.astype(jnp.int32)
    odd = (quarter & 1) == 1
    cosine = jnp.where(odd, s, c)
    sine = jnp.where(odd, c, s)
    cosine = jnp.where(((quarter + 1) & 2) == 2, -cosine, cosine)
    sine = jnp.where((quarter & 2) == 2, -sine, sine)
    return cosine, sine


def start_of(place, doc):
    start = jnp.zeros_like(place)
    for d in range(1, DOCS):
        start = jnp.where(place >= doc[d], doc[d], start)
    return start


def kernel(
    q_hbm, k_hbm, v_hbm, doc_hbm, qg_hbm, kg_hbm, out_ref,
    qb, kb, vb, doc, gains, stage, send_a, send_b, recv_a, recv_b, vt, probs, kpos, wq,
    back, gathered, rows_out,
    in_sem, send_sem, ra_sem, rb_sem, back_send, back_recv, from_below, from_above,
):
    seqa, seqb = lax.axis_index("seqa"), lax.axis_index("seqb")
    me = seqa * NB + seqb
    my_tile = seqa // 2
    core, chip_x, chip_z = lax.rem(seqa, 2), seqb // 2, lax.rem(seqb, 2) * 8 + my_tile
    across = [(chip_x, core)] + [
        (lax.rem(chip_x + i // 2, 4), lax.rem(core + i, 2)) for i in range(1, 8)
    ]

    def at_plane(z):
        z = lax.rem(z, 16)
        low, high = lax.rem(z, 8), z // 8
        return [
            (low * 16 + c * 8 + x * 2 + high, {"seqa": low * 2 + c, "seqb": x * 2 + high})
            for x, c in across
        ]

    with jax.named_scope("greet"):
        loads = [
            pltpu.make_async_copy(src, dst, in_sem.at[i])
            for i, (src, dst) in enumerate(
                (
                    (doc_hbm, doc), (qg_hbm, gains.at[0]), (kg_hbm, gains.at[1]),
                    (q_hbm, qb), (k_hbm, kb), (v_hbm, vb),
                )
            )
        ]
        for load in loads:
            load.start()
        barrier = pltpu.get_barrier_semaphore()
        above, below = at_plane(chip_z + 1)[0][1], at_plane(chip_z + 15)[0][1]
        for where in [at[1] for at in at_plane(chip_z)[1:]] + [above, below]:
            pl.semaphore_signal(barrier, inc=1, device_id=where, device_id_type=MESH)

    row = lax.broadcasted_iota(jnp.int32, (WIDTH // 2, HEADS), 0)
    freq = jnp.zeros((WIDTH // 2, HEADS), jnp.float32)
    for i, f in enumerate(FREQS):
        freq = jnp.where(row == i, jnp.float32(f), freq)
    with jax.named_scope("load"):
        for load in loads:
            load.wait()
    gq, gk = (
        jnp.transpose(jnp.broadcast_to(gains[i], (HEADS, WIDTH)), (1, 0)) for i in range(2)
    )
    place = me * TOK + lax.broadcasted_iota(jnp.int32, (1, HEADS), 1)
    cosines, sines = cos_sin((place - start_of(place, doc)).astype(jnp.float32) * freq)

    def prepared(x, gain, cosine, sine):
        x = x.astype(jnp.float32)
        mean = jnp.sum(x * x, axis=0, keepdims=True) * (1.0 / WIDTH)
        x = x * lax.rsqrt(mean + 1e-06) * gain
        a, b = x[: WIDTH // 2], x[WIDTH // 2 :]
        return a * cosine - b * sine, a * sine + b * cosine

    with jax.named_scope("prep"):
        for r in range(HALF):
            parts_q, parts_k, parts_v = [], [], []
            for t in (r, r + HALF):
                cosine, sine = (
                    jnp.broadcast_to(table[:, t : t + 1], (WIDTH // 2, HEADS))
                    for table in (cosines, sines)
                )
                parts_q.extend(prepared(qb[t], gq, cosine, sine))
                parts_k.extend(prepared(kb[t], gk, cosine, sine))
                parts_v.append(vb[t].astype(jnp.float32))
            for at, parts in ((0, parts_k), (HALF, parts_v), (2 * HALF, parts_q)):
                block = jnp.transpose(jnp.concatenate(parts, axis=0), (1, 0))
                stage[pl.ds(at + r, HEADS, stride=3 * HALF), :] = block

    def pack(h, carry):
        rows = stage[pl.ds(pl.multiple_of(h * 8 * 3 * HALF, 8), 8 * 3 * HALF), :]
        rows = rows.reshape(8, 3 * HALF, 2 * WIDTH)
        send_a[pl.ds(h * 8, 8)] = rows[:, : 2 * HALF + SUB].astype(jnp.bfloat16)
        send_b[pl.ds(h * 8, 8)] = rows[:, 2 * HALF + SUB :].astype(jnp.bfloat16)
        return carry

    with jax.named_scope("pack"):
        lax.fori_loop(0, HEADS // 8, pack, 0)

    def post(which, p, where):
        source, target, arrival = (
            (send_a, recv_a, ra_sem), (send_b, recv_b, rb_sem)
        )[which]
        pltpu.make_async_remote_copy(
            src_ref=source.at[p], dst_ref=target.at[me], send_sem=send_sem.at[which],
            recv_sem=arrival.at[my_tile], device_id=where, device_id_type=MESH,
        ).start()

    def post_mixed(which, spots):
        for i in spots:
            x, c = across[i]

            def one(k, carry):
                away = jnp.where(lax.rem(k, 2) == 1, 8 - (k + 1) // 2, 8 + k // 2)
                z = lax.rem(chip_z + away, 16)
                low, high = lax.rem(z, 8), z // 8
                post(
                    which, low * 16 + c * 8 + x * 2 + high,
                    {"seqa": low * 2 + c, "seqb": x * 2 + high},
                )
                return carry

            lax.fori_loop(0, 15 if i == 0 else 16, one, 0)

    def tell(sem, where):
        pl.semaphore_signal(sem, inc=1, device_id=where, device_id_type=MESH)

    with jax.named_scope("barrier"):
        pl.semaphore_wait(barrier, 9)
    near = 4
    with jax.named_scope("post_a"):
        tell(from_below.at[1], above)
        tell(from_above.at[1], below)
        for at in at_plane(chip_z)[1:near]:
            post(0, *at)

        def ring(k, carry):
            pl.semaphore_wait(from_below.at[k], 1)
            tell(from_below.at[k + 1], above)
            pl.semaphore_wait(from_above.at[k], 1)

            @pl.when(k < 7)
            def _():
                tell(from_above.at[k + 1], below)

            for at in at_plane(chip_z + 16 - k)[:near] + at_plane(chip_z + k)[:near]:
                post(0, *at)
            return carry

        lax.fori_loop(1, 8, ring, 0)
        pl.semaphore_wait(from_below.at[8], 1)
        for at in at_plane(chip_z + 8)[:near]:
            post(0, *at)
        post_mixed(0, range(near, 8))
    with jax.named_scope("post_b"):
        post_mixed(1, range(8))
    own_a = pltpu.make_async_copy(send_a.at[me], recv_a.at[me], ra_sem.at[my_tile])
    own_b = pltpu.make_async_copy(send_b.at[me], recv_b.at[me], rb_sem.at[my_tile])
    own_a.start()
    own_b.start()

    def others(ref):
        part = ref.at[pl.ds(1, N - 1)]
        return part, part

    key_row = lax.broadcasted_iota(jnp.int32, (PER * HALF, 2 * WIDTH), 0)
    kpos[...] = lax.rem(key_row, HALF) + (key_row // HALF) * TOK

    def arrived(ref, sem, j):
        part = ref.at[pl.ds(j * PER, PER)]
        pltpu.make_async_copy(part, part, sem.at[j]).wait()

    with jax.named_scope("wait_a"):
        for j in range(TILES):
            arrived(recv_a, ra_sem, j)
    for j in range(TILES):
        v = recv_a[j * PER : (j + 1) * PER, HALF : 2 * HALF, :].reshape(PER * HALF, 2 * WIDTH)
        v = jnp.transpose(v.astype(jnp.float32), (1, 0)).astype(jnp.bfloat16)
        vt[j, :, : PER * HALF] = v[:WIDTH]
        vt[j, :, PER * HALF :] = v[WIDTH:]

    low = lax.broadcasted_iota(jnp.int32, (PER * SUB, 2 * WIDTH), 1) < WIDTH
    queries = 2 * PER * SUB
    span = PER * TOK

    def tile(i, g):
        if g == 0:
            x = recv_a[i * PER : (i + 1) * PER, 2 * HALF :, :]
        else:
            x = recv_b[i * PER : (i + 1) * PER]
        x = x.astype(jnp.float32).reshape(PER * SUB, 2 * WIDTH)
        turned = pltpu.roll(x, WIDTH, 1)
        zero = jnp.zeros_like(x)
        wq[0, : PER * SUB] = jnp.where(low, x, zero).astype(jnp.bfloat16)
        wq[0, PER * SUB :] = jnp.where(low, turned, zero).astype(jnp.bfloat16)
        wq[1, : PER * SUB] = jnp.where(low, zero, turned).astype(jnp.bfloat16)
        wq[1, PER * SUB :] = jnp.where(low, zero, x).astype(jnp.bfloat16)
        lane = lax.broadcasted_iota(jnp.int32, (1, queries), 1)
        within = lax.rem(lane, PER * SUB)
        place = (
            i * span + (within // SUB) * TOK + lax.rem(within, SUB) + g * SUB
            + jnp.where(lane >= PER * SUB, HALF, 0)
        )
        start = start_of(place, doc)
        total = jnp.zeros((8, queries), jnp.float32)
        for j in range(i + 1):
            keys = recv_a[j * PER : (j + 1) * PER, :HALF, :].reshape(PER * HALF, 2 * WIDTH)
            for half in range(2):
                scores = lax.dot_general(
                    keys, wq[half], (((1,), (1,)), ((), ())), preferred_element_type=jnp.float32
                )
                at = jnp.concatenate([kpos[...], kpos[...]], axis=1)
                base = j * span + half * HALF
                allowed = at >= start - base
                if j == i:
                    allowed = allowed & (at <= place - base)
                p = jnp.where(allowed, jnp.exp2(scores * SCALE), 0.0)
                probs[j, half * PER * HALF : (half + 1) * PER * HALF] = p
                total = total + jnp.sum(p.reshape(PER * HALF // 8, 8, queries), axis=0)
        inverse = 1.0 / jnp.sum(total, axis=0, keepdims=True)
        out = jnp.zeros((WIDTH, queries), jnp.float32)
        for j in range(i + 1):
            weights = (probs[j] * inverse).astype(jnp.bfloat16)
            out = out + jnp.dot(vt[j], weights, preferred_element_type=jnp.float32)
        out = jnp.concatenate([out[:, : PER * SUB], out[:, PER * SUB :]], axis=0)
        out = jnp.transpose(out, (1, 0)).reshape(PER, SUB, 2 * WIDTH)
        back[g, i * PER : (i + 1) * PER] = out.astype(jnp.bfloat16)
        for p in range(i * PER, (i + 1) * PER):

            @pl.when(p != me)
            def _():
                pltpu.make_async_remote_copy(
                    src_ref=back.at[g, p], dst_ref=gathered.at[g, me], send_sem=back_send.at[g],
                    recv_sem=back_recv.at[g], device_id={"seqa": p // NB, "seqb": p % NB},
                    device_id_type=MESH,
                ).start()

    for g in range(2):
        if g == 1:
            with jax.named_scope("wait_b"):
                for j in range(TILES):
                    arrived(recv_b, rb_sem, j)

        def step(t, carry):
            i = lax.rem(my_tile + jnp.where(lax.rem(t, 2) == 1, TILES - (t + 1) // 2, t // 2), TILES)
            lax.switch(i, [functools.partial(tile, k, g) for k in range(TILES)])
            return carry

        with jax.named_scope(f"tiles_{g}"):
            lax.fori_loop(0, TILES, step, 0)

    for g in range(2):
        gathered[g, me] = back[g, me]
        with jax.named_scope(f"wait_back_{g}"):
            pltpu.make_async_copy(*others(gathered.at[g]), back_recv.at[g]).wait()
        rows_out[...] = gathered[g].astype(jnp.float32).reshape(HEADS * SUB, 2 * WIDTH)
        for r in range(SUB):
            block = jnp.transpose(rows_out[pl.ds(r, HEADS, stride=SUB), :], (1, 0))
            block = block.astype(jnp.bfloat16)
            out_ref[g * SUB + r] = block[:WIDTH]
            out_ref[g * SUB + r + HALF] = block[WIDTH:]
    pltpu.make_async_copy(*others(send_a), send_sem.at[0]).wait()
    pltpu.make_async_copy(*others(send_b), send_sem.at[1]).wait()
    for g in range(2):
        pltpu.make_async_copy(*others(back.at[g]), back_send.at[g]).wait()


def attention(queries, keys, values, doc_bounds, q_gain, k_gain):
    tok, heads, width = queries.shape
    assert (tok, heads, width) == (TOK, HEADS, WIDTH)
    queries, keys, values = (jnp.transpose(a, (0, 2, 1)) for a in (queries, keys, values))
    block = pltpu.VMEM((TOK, WIDTH, HEADS), jnp.bfloat16)
    bf16, f32 = jnp.bfloat16, jnp.float32
    dma = pltpu.SemaphoreType.DMA
    out = pl.pallas_call(
        kernel,
        out_shape=jax.ShapeDtypeStruct((TOK, WIDTH, HEADS), bf16),
        in_specs=[pl.BlockSpec(memory_space=pl.ANY)] * 6,
        out_specs=pl.BlockSpec(memory_space=pltpu.VMEM),
        scratch_shapes=[
            block, block, block,
            pltpu.SMEM(doc_bounds.shape, jnp.int32),
            pltpu.VMEM((2, 1, WIDTH), f32),
            pltpu.VMEM((HEADS * 3 * HALF, 2 * WIDTH), f32),
            pltpu.VMEM((N, 2 * HALF + SUB, 2 * WIDTH), bf16),
            pltpu.VMEM((N, SUB, 2 * WIDTH), bf16),
            pltpu.VMEM((N, 2 * HALF + SUB, 2 * WIDTH), bf16),
            pltpu.VMEM((N, SUB, 2 * WIDTH), bf16),
            pltpu.VMEM((TILES, WIDTH, 2 * PER * HALF), bf16),
            pltpu.VMEM((TILES, 2 * PER * HALF, 2 * PER * SUB), f32),
            pltpu.VMEM((PER * HALF, 2 * WIDTH), jnp.int32),
            pltpu.VMEM((2, 2 * PER * SUB, 2 * WIDTH), bf16),
            pltpu.VMEM((2, N, SUB, 2 * WIDTH), bf16),
            pltpu.VMEM((2, N, SUB, 2 * WIDTH), bf16),
            pltpu.VMEM((HEADS * SUB, 2 * WIDTH), f32),
            dma((6,)), dma((2,)), dma((TILES,)), dma((TILES,)), dma((2,)), dma((2,)),
            pltpu.SemaphoreType.REGULAR((9,)), pltpu.SemaphoreType.REGULAR((8,)),
        ],
        compiler_params=pltpu.CompilerParams(
            collective_id=0, has_side_effects=True, vmem_limit_bytes=60 << 20
        ),
    )(queries, keys, values, doc_bounds, q_gain.reshape(1, WIDTH), k_gain.reshape(1, WIDTH))
    return jnp.transpose(out, (0, 2, 1))


def solution(mesh):
    assert mesh.shape["seqa"] * mesh.shape["seqb"] == N and mesh.shape["seqb"] == NB
    rows = P(("dp", "seqa", "seqb"), None, None)
    return jax.shard_map(
        attention,
        mesh=mesh,
        in_specs=(rows, rows, rows, P("dp"), P(), P()),
        out_specs=rows,
        check_vma=False,
    )
```

```python
import functools
import math

import jax
import jax.numpy as jnp
import numpy as np
from jax import lax
from jax.experimental import pallas as pl
from jax.experimental.pallas import tpu as pltpu
from jax.sharding import PartitionSpec as P

MESH = pl.DeviceIdType.MESH
DOCS = 8
TOK, HEADS, WIDTH = 32, 128, 64
N, NB = 128, 8
HALF = TOK // 2
SUB = HALF // 2
TILES = 8
PER = N // TILES
FAR = -2048.0
SCALE = math.log2(math.e) / math.sqrt(WIDTH)
LOG_BASE = np.float32(-np.log(np.float32(10000.0)))
FREQS = [
    float(np.float32(np.exp(np.float64(np.float32(LOG_BASE * np.float32(i)) * 2.0 / WIDTH))))
    for i in range(WIDTH // 2)
]


def cos_sin(angle):
    turns = jnp.floor(angle * 0.6366197723675814 + 0.5)
    r = angle - turns * 1.5703125
    r = r - turns * 4.837512969970703125e-4
    r = r - turns * 7.54978995489188216e-8
    z = r * r
    s = ((-1.9515295891e-4 * z + 8.3321608736e-3) * z - 1.6666654611e-1) * z * r + r
    c = ((2.443315711809948e-5 * z - 1.388731625493765e-3) * z + 4.166664568298827e-2) * z * z
    c = c - 0.5 * z + 1.0
    quarter = turns.astype(jnp.int32)
    odd = (quarter & 1) == 1
    cosine = jnp.where(odd, s, c)
    sine = jnp.where(odd, c, s)
    cosine = jnp.where(((quarter + 1) & 2) == 2, -cosine, cosine)
    sine = jnp.where((quarter & 2) == 2, -sine, sine)
    return cosine, sine


def start_of(place, doc):
    start = jnp.zeros_like(place)
    for d in range(1, DOCS):
        start = jnp.where(place >= doc[d], doc[d], start)
    return start


def kernel(
    q_hbm, k_hbm, v_hbm, doc_hbm, qg_hbm, kg_hbm, out_ref,
    qb, kb, vb, doc, gains, stage, send_a, send_b, recv_a, recv_b, kx, vt, probs_a, probs_b, kpos, qpos,
    wq,    back, gathered, rows_out,
    in_sem, send_sem, ra_sem, rb_sem, back_send, back_recv, from_below, from_above,
):
    seqa, seqb = lax.axis_index("seqa"), lax.axis_index("seqb")
    me = seqa * NB + seqb
    my_tile = seqa // 2
    core, chip_x, chip_z = lax.rem(seqa, 2), seqb // 2, lax.rem(seqb, 2) * 8 + my_tile
    across = [(chip_x, core)] + [
        (lax.rem(chip_x + i // 2, 4), lax.rem(core + i, 2)) for i in range(1, 8)
    ]

    def at_plane(z):
        z = lax.rem(z, 16)
        low, high = lax.rem(z, 8), z // 8
        return [
            (low * 16 + c * 8 + x * 2 + high, {"seqa": low * 2 + c, "seqb": x * 2 + high})
            for x, c in across
        ]

    with jax.named_scope("greet"):
        loads = [
            pltpu.make_async_copy(src, dst, in_sem.at[i])
            for i, (src, dst) in enumerate(
                (
                    (doc_hbm, doc), (qg_hbm, gains.at[0]), (kg_hbm, gains.at[1]),
                    (q_hbm, qb), (k_hbm, kb), (v_hbm, vb),
                )
            )
        ]
        for load in loads:
            load.start()
        barrier = pltpu.get_barrier_semaphore()
        above, below = at_plane(chip_z + 1)[0][1], at_plane(chip_z + 15)[0][1]
        for where in [at[1] for at in at_plane(chip_z)[1:]] + [above, below]:
            pl.semaphore_signal(barrier, inc=1, device_id=where, device_id_type=MESH)

    row = lax.broadcasted_iota(jnp.int32, (WIDTH // 2, HEADS), 0)
    freq = jnp.zeros((WIDTH // 2, HEADS), jnp.float32)
    for i, f in enumerate(FREQS):
        freq = jnp.where(row == i, jnp.float32(f), freq)
    with jax.named_scope("load"):
        for load in loads:
            load.wait()
    gq, gk = (
        jnp.transpose(jnp.broadcast_to(gains[i], (HEADS, WIDTH)), (1, 0)) for i in range(2)
    )
    place = me * TOK + lax.broadcasted_iota(jnp.int32, (1, HEADS), 1)
    cosines, sines = cos_sin((place - start_of(place, doc)).astype(jnp.float32) * freq)

    def prepared(x, gain, cosine, sine):
        x = x.astype(jnp.float32)
        mean = jnp.sum(x * x, axis=0, keepdims=True) * (1.0 / WIDTH)
        x = x * lax.rsqrt(mean + 1e-06) * gain
        a, b = x[: WIDTH // 2], x[WIDTH // 2 :]
        return a * cosine - b * sine, a * sine + b * cosine

    with jax.named_scope("prep"):
        for r in range(HALF):
            parts_q, parts_k, parts_v = [], [], []
            for t in (r, r + HALF):
                cosine, sine = (
                    jnp.broadcast_to(table[:, t : t + 1], (WIDTH // 2, HEADS))
                    for table in (cosines, sines)
                )
                parts_q.extend(prepared(qb[t], gq, cosine, sine))
                parts_k.extend(prepared(kb[t], gk, cosine, sine))
                parts_v.append(vb[t].astype(jnp.float32))
            for at, parts in ((0, parts_k), (HALF, parts_v), (2 * HALF, parts_q)):
                block = jnp.transpose(jnp.concatenate(parts, axis=0), (1, 0))
                stage[pl.ds(at + r, HEADS, stride=3 * HALF), :] = block

    def pack(h, carry):
        rows = stage[pl.ds(pl.multiple_of(h * 8 * 3 * HALF, 8), 8 * 3 * HALF), :]
        rows = rows.reshape(8, 3 * HALF, 2 * WIDTH)
        send_a[pl.ds(h * 8, 8)] = rows[:, : 2 * HALF + SUB].astype(jnp.bfloat16)
        send_b[pl.ds(h * 8, 8)] = rows[:, 2 * HALF + SUB :].astype(jnp.bfloat16)
        return carry

    with jax.named_scope("pack"):
        lax.fori_loop(0, HEADS // 8, pack, 0)

    def post(which, p, where):
        source, target, arrival = (
            (send_a, recv_a, ra_sem), (send_b, recv_b, rb_sem)
        )[which]
        pltpu.make_async_remote_copy(
            src_ref=source.at[p], dst_ref=target.at[me], send_sem=send_sem.at[which],
            recv_sem=arrival.at[my_tile], device_id=where, device_id_type=MESH,
        ).start()

    def post_mixed(which, spots):
        for i in spots:
            x, c = across[i]

            def one(k, carry):
                away = jnp.where(lax.rem(k, 2) == 1, 8 - (k + 1) // 2, 8 + k // 2)
                z = lax.rem(chip_z + away, 16)
                low, high = lax.rem(z, 8), z // 8
                post(
                    which, low * 16 + c * 8 + x * 2 + high,
                    {"seqa": low * 2 + c, "seqb": x * 2 + high},
                )
                return carry

            lax.fori_loop(0, 15 if i == 0 else 16, one, 0)

    def tell(sem, where):
        pl.semaphore_signal(sem, inc=1, device_id=where, device_id_type=MESH)

    with jax.named_scope("barrier"):
        pl.semaphore_wait(barrier, 9)
    near = 4
    with jax.named_scope("post_a"):
        tell(from_below.at[1], above)
        tell(from_above.at[1], below)
        for at in at_plane(chip_z)[1:near]:
            post(0, *at)

        def ring(k, carry):
            pl.semaphore_wait(from_below.at[k], 1)
            tell(from_below.at[k + 1], above)
            pl.semaphore_wait(from_above.at[k], 1)

            @pl.when(k < 7)
            def _():
                tell(from_above.at[k + 1], below)

            for at in at_plane(chip_z + 16 - k)[:near] + at_plane(chip_z + k)[:near]:
                post(0, *at)
            return carry

        lax.fori_loop(1, 8, ring, 0)
        pl.semaphore_wait(from_below.at[8], 1)
        for at in at_plane(chip_z + 8)[:near]:
            post(0, *at)
        post_mixed(0, range(near, 8))
    with jax.named_scope("post_b"):
        post_mixed(1, range(8))
    own_a = pltpu.make_async_copy(send_a.at[me], recv_a.at[me], ra_sem.at[my_tile])
    own_b = pltpu.make_async_copy(send_b.at[me], recv_b.at[me], rb_sem.at[my_tile])
    own_a.start()
    own_b.start()

    def others(ref):
        part = ref.at[pl.ds(1, N - 1)]
        return part, part

    def arrived(ref, sem, j):
        part = ref.at[pl.ds(pl.multiple_of(j * PER, PER), PER)]
        pltpu.make_async_copy(part, part, sem.at[j]).wait()

    queries, span, keys = 2 * PER * SUB, PER * TOK, PER * HALF
    lane = lax.broadcasted_iota(jnp.int32, (1, 2 * WIDTH), 1)
    mark = lax.rem(lane, WIDTH)
    first_of, end_of = jnp.full_like(lane, TILES * span), jnp.zeros_like(lane)
    for d in range(DOCS):
        first_of = jnp.where(mark == d, doc[d], first_of)
        end_of = jnp.where(mark == d, doc[d + 1], end_of)
    low = lane < WIDTH
    key_row = lax.broadcasted_iota(jnp.int32, (keys, 2 * WIDTH), 0)
    kpos[...] = lax.rem(key_row, HALF) + (key_row // HALF) * TOK
    query_row = lax.broadcasted_iota(jnp.int32, (PER * SUB, 2 * WIDTH), 0)
    qpos[...] = lax.rem(query_row, SUB) + (query_row // SUB) * TOK

    def marks(at, same, other):
        return jnp.where((at >= first_of) & (at < end_of), same, other)

    def take_keys(j):
        both = recv_a[pl.ds(j * PER, PER), : 2 * HALF, :]
        k = both[:, :HALF].reshape(keys, 2 * WIDTH)
        one, zero = jnp.float32(1.0), jnp.float32(0.0)
        for half in range(2):
            own = low if half == 0 else jnp.logical_not(low)
            at = kpos[...] + (j * span + half * HALF)
            marked = jnp.where(own, k.astype(jnp.float32), marks(at, one, zero))
            kx[half, j] = marked.astype(jnp.bfloat16)
        v = both[:, HALF:].reshape(keys, 2 * WIDTH)
        v = jnp.transpose(v.astype(jnp.float32), (1, 0)).astype(jnp.bfloat16)
        vt[j, :, :keys] = v[:WIDTH]
        vt[j, :, keys:] = v[WIDTH:]

    def take_queries(i, g):
        if g == 0:
            x = recv_a[pl.ds(i * PER, PER), 2 * HALF :, :]
        else:
            x = recv_b[pl.ds(i * PER, PER)]
        x = x.astype(jnp.float32).reshape(PER * SUB, 2 * WIDTH)
        turned = pltpu.roll(x, WIDTH, 1)
        for late in range(2):
            at = qpos[...] + (i * span + g * SUB + late * HALF)
            m = marks(at, jnp.float32(0.0), jnp.float32(FAR))
            rows = pl.ds(late * PER * SUB, PER * SUB)
            first, second = (x, turned) if late == 0 else (turned, x)
            wq[0, i, rows] = jnp.where(low, first, m).astype(jnp.bfloat16)
            wq[1, i, rows] = jnp.where(low, m, second).astype(jnp.bfloat16)

    def scores_of(i, g, probs):
        spot = lax.broadcasted_iota(jnp.int32, (1, queries), 1)
        within = lax.rem(spot, PER * SUB)
        place = (
            (within // SUB) * TOK + lax.rem(within, SUB) + g * SUB
            + jnp.where(spot >= PER * SUB, HALF, 0)
        )
        total = jnp.zeros((16, queries), jnp.float32)
        for j in range(i + 1):
            for half in range(2):
                p = lax.dot_general(
                    kx[half, j], wq[half, i], (((1,), (1,)), ((), ())),
                    preferred_element_type=jnp.float32,
                )
                p = jnp.exp2(p * SCALE)
                if j == i:
                    at = jnp.concatenate([kpos[...], kpos[...]], axis=1)
                    p = jnp.where(at <= place - half * HALF, p, 0.0)
                probs[j, half * keys : (half + 1) * keys] = p
                total = total + jnp.sum(p.reshape(keys // 16, 16, queries), axis=0)
        return 1.0 / jnp.sum(total, axis=0, keepdims=True)

    def outputs_of(i, g, probs, inverse):
        out = jnp.zeros((WIDTH, queries), jnp.float32)
        for j in range(i + 1):
            weights = (probs[j] * inverse).astype(jnp.bfloat16)
            out = out + jnp.dot(vt[j], weights, preferred_element_type=jnp.float32)
        out = jnp.concatenate([out[:, : PER * SUB], out[:, PER * SUB :]], axis=0)
        out = jnp.transpose(out, (1, 0)).reshape(PER, SUB, 2 * WIDTH)
        back[g, i * PER : (i + 1) * PER] = out.astype(jnp.bfloat16)

    def send_home(i, g, high, c, x):
        p = i * PER + c * NB + x * 2 + high

        @pl.when(p != me)
        def _():
            pltpu.make_async_remote_copy(
                src_ref=back.at[g, p], dst_ref=gathered.at[g, me], send_sem=back_send.at[g],
                recv_sem=back_recv.at[g], device_id={"seqa": 2 * i + c, "seqb": x * 2 + high},
                device_id_type=MESH,
            ).start()

    def pair(first, g):
        second = first + TILES // 2
        small = scores_of(first, g, probs_a)
        large = scores_of(second, g, probs_b)
        outputs_of(first, g, probs_a, small)
        outputs_of(second, g, probs_b, large)
        for c in range(2):
            for x in range(4):
                send_home(first, g, 0, c, x)
                send_home(second, g, 0, c, x)

    def late_half(t, g):
        i = lax.rem(my_tile + jnp.where(lax.rem(t, 2) == 1, TILES - (t + 1) // 2, t // 2), TILES)
        for c in range(2):
            for x in range(4):
                send_home(i, g, 1, c, x)

    def come_in(j, carry):
        arrived(recv_a, ra_sem, j)
        take_keys(j)
        take_queries(j, 0)
        return carry

    def come_in_b(j, carry):
        arrived(recv_b, rb_sem, j)
        take_queries(j, 1)
        return carry

    for g in range(2):
        with jax.named_scope(f"wait_{g}"):
            lax.fori_loop(0, TILES, come_in if g == 0 else come_in_b, 0)

        def step(t, carry):
            away = jnp.where(t >= 2, 5 - t, t)
            i = lax.rem(my_tile + away, TILES // 2)
            lax.switch(i, [functools.partial(pair, k, g) for k in range(TILES // 2)])
            return carry

        with jax.named_scope(f"tiles_{g}"):
            lax.fori_loop(0, TILES // 2, step, 0)

        def rest(t, carry):
            late_half(t, g)
            return carry

        with jax.named_scope(f"rest_{g}"):
            lax.fori_loop(0, TILES, rest, 0)

    for g in range(2):
        gathered[g, me] = back[g, me]
        with jax.named_scope(f"wait_back_{g}"):
            pltpu.make_async_copy(*others(gathered.at[g]), back_recv.at[g]).wait()
        rows_out[...] = gathered[g].astype(jnp.float32).reshape(HEADS * SUB, 2 * WIDTH)
        for r in range(SUB):
            block = jnp.transpose(rows_out[pl.ds(r, HEADS, stride=SUB), :], (1, 0))
            block = block.astype(jnp.bfloat16)
            out_ref[g * SUB + r] = block[:WIDTH]
            out_ref[g * SUB + r + HALF] = block[WIDTH:]
    pltpu.make_async_copy(*others(send_a), send_sem.at[0]).wait()
    pltpu.make_async_copy(*others(send_b), send_sem.at[1]).wait()
    for g in range(2):
        pltpu.make_async_copy(*others(back.at[g]), back_send.at[g]).wait()


def attention(queries, keys, values, doc_bounds, q_gain, k_gain):
    tok, heads, width = queries.shape
    assert (tok, heads, width) == (TOK, HEADS, WIDTH)
    queries, keys, values = (jnp.transpose(a, (0, 2, 1)) for a in (queries, keys, values))
    block = pltpu.VMEM((TOK, WIDTH, HEADS), jnp.bfloat16)
    bf16, f32 = jnp.bfloat16, jnp.float32
    dma = pltpu.SemaphoreType.DMA
    out = pl.pallas_call(
        kernel,
        out_shape=pltpu.VMEM((TOK, WIDTH, HEADS), bf16),
        in_specs=[pl.BlockSpec(memory_space=pl.ANY)] * 6,
        out_specs=pl.BlockSpec(memory_space=pltpu.VMEM),
        scratch_shapes=[
            block, block, block,
            pltpu.SMEM(doc_bounds.shape, jnp.int32),
            pltpu.VMEM((2, 1, WIDTH), f32),
            pltpu.VMEM((HEADS * 3 * HALF, 2 * WIDTH), f32),
            pltpu.VMEM((N, 2 * HALF + SUB, 2 * WIDTH), bf16),
            pltpu.VMEM((N, SUB, 2 * WIDTH), bf16),
            pltpu.VMEM((N, 2 * HALF + SUB, 2 * WIDTH), bf16),
            pltpu.VMEM((N, SUB, 2 * WIDTH), bf16),
            pltpu.VMEM((2, TILES, PER * HALF, 2 * WIDTH), bf16),
            pltpu.VMEM((TILES, WIDTH, 2 * PER * HALF), bf16),
            pltpu.VMEM((TILES // 2, 2 * PER * HALF, 2 * PER * SUB), f32),
            pltpu.VMEM((TILES, 2 * PER * HALF, 2 * PER * SUB), f32),
            pltpu.VMEM((PER * HALF, 2 * WIDTH), jnp.int32),
            pltpu.VMEM((PER * SUB, 2 * WIDTH), jnp.int32),
            pltpu.VMEM((2, TILES, 2 * PER * SUB, 2 * WIDTH), bf16),
            pltpu.VMEM((2, N, SUB, 2 * WIDTH), bf16),
            pltpu.VMEM((2, N, SUB, 2 * WIDTH), bf16),
            pltpu.VMEM((HEADS * SUB, 2 * WIDTH), f32),
            dma((6,)), dma((2,)), dma((TILES,)), dma((TILES,)), dma((2,)), dma((2,)),
            pltpu.SemaphoreType.REGULAR((9,)), pltpu.SemaphoreType.REGULAR((8,)),
        ],
        compiler_params=pltpu.CompilerParams(
            collective_id=0, has_side_effects=True, vmem_limit_bytes=60 << 20
        ),
    )(queries, keys, values, doc_bounds, q_gain.reshape(1, WIDTH), k_gain.reshape(1, WIDTH))
    return jnp.transpose(out, (0, 2, 1))


def solution(mesh):
    assert mesh.shape["seqa"] * mesh.shape["seqb"] == N and mesh.shape["seqb"] == NB
    rows = P(("dp", "seqa", "seqb"), None, None)
    return jax.shard_map(
        attention,
        mesh=mesh,
        in_specs=(rows, rows, rows, P("dp"), P(), P()),
        out_specs=rows,
        check_vma=False,
    )
```

```python
import functools
import math

import jax
import jax.numpy as jnp
import numpy as np
from jax import lax
from jax.experimental import pallas as pl
from jax.experimental.pallas import tpu as pltpu
from jax.sharding import PartitionSpec as P

MESH = pl.DeviceIdType.MESH
DOCS = 8
TOK, HEADS, WIDTH = 32, 128, 64
N, NB = 128, 8
HALF = TOK // 2
SUB = HALF // 2
TILES = 8
PER = N // TILES
FAR = -2048.0
SCALE = math.log2(math.e) / math.sqrt(WIDTH)
LOG_BASE = np.float32(-np.log(np.float32(10000.0)))
FREQS = [
    float(np.float32(np.exp(np.float64(np.float32(LOG_BASE * np.float32(i)) * 2.0 / WIDTH))))
    for i in range(WIDTH // 2)
]


def cos_sin(angle):
    turns = jnp.floor(angle * 0.6366197723675814 + 0.5)
    r = angle - turns * 1.5703125
    r = r - turns * 4.837512969970703125e-4
    r = r - turns * 7.54978995489188216e-8
    z = r * r
    s = ((-1.9515295891e-4 * z + 8.3321608736e-3) * z - 1.6666654611e-1) * z * r + r
    c = ((2.443315711809948e-5 * z - 1.388731625493765e-3) * z + 4.166664568298827e-2) * z * z
    c = c - 0.5 * z + 1.0
    quarter = turns.astype(jnp.int32)
    odd = (quarter & 1) == 1
    cosine = jnp.where(odd, s, c)
    sine = jnp.where(odd, c, s)
    cosine = jnp.where(((quarter + 1) & 2) == 2, -cosine, cosine)
    sine = jnp.where((quarter & 2) == 2, -sine, sine)
    return cosine, sine


def start_of(place, doc):
    start = jnp.zeros_like(place)
    for d in range(1, DOCS):
        start = jnp.where(place >= doc[d], doc[d], start)
    return start


def kernel(
    q_hbm, k_hbm, v_hbm, doc_hbm, qg_hbm, kg_hbm, out_ref,
    qb, kb, vb, doc, gains, stage, send_a, send_b, recv_a, recv_b, kx, vt, probs_a, probs_b, kpos, qpos,
    wq,    back, gathered, rows_out,
    in_sem, send_sem, ra_sem, rb_sem, back_send, back_recv, from_below, from_above,
):
    seqa, seqb = lax.axis_index("seqa"), lax.axis_index("seqb")
    me = seqa * NB + seqb
    my_tile = seqa // 2
    core, chip_x, chip_z = lax.rem(seqa, 2), seqb // 2, lax.rem(seqb, 2) * 8 + my_tile
    across = [(chip_x, core)] + [
        (lax.rem(chip_x + i // 2, 4), lax.rem(core + i, 2)) for i in range(1, 8)
    ]

    def at_plane(z):
        z = lax.rem(z, 16)
        low, high = lax.rem(z, 8), z // 8
        return [
            (low * 16 + c * 8 + x * 2 + high, {"seqa": low * 2 + c, "seqb": x * 2 + high})
            for x, c in across
        ]

    with jax.named_scope("greet"):
        loads = [
            pltpu.make_async_copy(src, dst, in_sem.at[i])
            for i, (src, dst) in enumerate(
                (
                    (doc_hbm, doc), (qg_hbm, gains.at[0]), (kg_hbm, gains.at[1]),
                    (q_hbm, qb), (k_hbm, kb), (v_hbm, vb),
                )
            )
        ]
        for load in loads:
            load.start()
        barrier = pltpu.get_barrier_semaphore()
        above, below = at_plane(chip_z + 1)[0][1], at_plane(chip_z + 15)[0][1]
        for where in [at[1] for at in at_plane(chip_z)[1:]] + [above, below]:
            pl.semaphore_signal(barrier, inc=1, device_id=where, device_id_type=MESH)

    row = lax.broadcasted_iota(jnp.int32, (WIDTH // 2, HEADS), 0)
    freq = jnp.zeros((WIDTH // 2, HEADS), jnp.float32)
    for i, f in enumerate(FREQS):
        freq = jnp.where(row == i, jnp.float32(f), freq)
    with jax.named_scope("load"):
        for load in loads:
            load.wait()
    gq, gk = (
        jnp.transpose(jnp.broadcast_to(gains[i], (HEADS, WIDTH)), (1, 0)) for i in range(2)
    )
    place = me * TOK + lax.broadcasted_iota(jnp.int32, (1, HEADS), 1)
    cosines, sines = cos_sin((place - start_of(place, doc)).astype(jnp.float32) * freq)

    def prepared(x, gain, cosine, sine):
        x = x.astype(jnp.float32)
        mean = jnp.sum(x * x, axis=0, keepdims=True) * (1.0 / WIDTH)
        x = x * lax.rsqrt(mean + 1e-06) * gain
        a, b = x[: WIDTH // 2], x[WIDTH // 2 :]
        return a * cosine - b * sine, a * sine + b * cosine

    with jax.named_scope("prep"):
        for r in range(HALF):
            parts_q, parts_k, parts_v = [], [], []
            for t in (r, r + HALF):
                cosine, sine = (
                    jnp.broadcast_to(table[:, t : t + 1], (WIDTH // 2, HEADS))
                    for table in (cosines, sines)
                )
                parts_q.extend(prepared(qb[t], gq, cosine, sine))
                parts_k.extend(prepared(kb[t], gk, cosine, sine))
                parts_v.append(vb[t].astype(jnp.float32))
            for at, parts in ((0, parts_k), (HALF, parts_v), (2 * HALF, parts_q)):
                block = jnp.transpose(jnp.concatenate(parts, axis=0), (1, 0))
                stage[pl.ds(at + r, HEADS, stride=3 * HALF), :] = block

    def pack(h, carry):
        rows = stage[pl.ds(pl.multiple_of(h * 8 * 3 * HALF, 8), 8 * 3 * HALF), :]
        rows = rows.reshape(8, 3 * HALF, 2 * WIDTH)
        send_a[pl.ds(h * 8, 8)] = rows[:, : 2 * HALF + SUB].astype(jnp.bfloat16)
        send_b[pl.ds(h * 8, 8)] = rows[:, 2 * HALF + SUB :].astype(jnp.bfloat16)
        return carry

    with jax.named_scope("pack"):
        lax.fori_loop(0, HEADS // 8, pack, 0)

    def post(which, p, where):
        source, target, arrival = (
            (send_a, recv_a, ra_sem), (send_b, recv_b, rb_sem)
        )[which]
        pltpu.make_async_remote_copy(
            src_ref=source.at[p], dst_ref=target.at[me], send_sem=send_sem.at[which],
            recv_sem=arrival.at[my_tile], device_id=where, device_id_type=MESH,
        ).start()

    def post_mixed(which, spots):
        for i in spots:
            x, c = across[i]

            def one(k, carry):
                away = jnp.where(lax.rem(k, 2) == 1, 8 - (k + 1) // 2, 8 + k // 2)
                z = lax.rem(chip_z + away, 16)
                low, high = lax.rem(z, 8), z // 8
                post(
                    which, low * 16 + c * 8 + x * 2 + high,
                    {"seqa": low * 2 + c, "seqb": x * 2 + high},
                )
                return carry

            lax.fori_loop(0, 15 if i == 0 else 16, one, 0)

    def tell(sem, where):
        pl.semaphore_signal(sem, inc=1, device_id=where, device_id_type=MESH)

    with jax.named_scope("barrier"):
        pl.semaphore_wait(barrier, 9)
    near = 4
    with jax.named_scope("post_a"):
        tell(from_below.at[1], above)
        tell(from_above.at[1], below)
        for at in at_plane(chip_z)[1:near]:
            post(0, *at)

        def ring(k, carry):
            pl.semaphore_wait(from_below.at[k], 1)
            tell(from_below.at[k + 1], above)
            pl.semaphore_wait(from_above.at[k], 1)

            @pl.when(k < 7)
            def _():
                tell(from_above.at[k + 1], below)

            for at in at_plane(chip_z + 16 - k)[:near] + at_plane(chip_z + k)[:near]:
                post(0, *at)
            return carry

        lax.fori_loop(1, 8, ring, 0)
        pl.semaphore_wait(from_below.at[8], 1)
        for at in at_plane(chip_z + 8)[:near]:
            post(0, *at)
        post_mixed(0, range(near, 8))
    with jax.named_scope("post_b"):
        post_mixed(1, range(8))
    own_a = pltpu.make_async_copy(send_a.at[me], recv_a.at[me], ra_sem.at[my_tile])
    own_b = pltpu.make_async_copy(send_b.at[me], recv_b.at[me], rb_sem.at[my_tile])
    own_a.start()
    own_b.start()

    def others(ref):
        part = ref.at[pl.ds(1, N - 1)]
        return part, part

    def arrived(ref, sem, j):
        part = ref.at[pl.ds(pl.multiple_of(j * PER, PER), PER)]
        pltpu.make_async_copy(part, part, sem.at[j]).wait()

    queries, span, keys = 2 * PER * SUB, PER * TOK, PER * HALF
    lane = lax.broadcasted_iota(jnp.int32, (1, 2 * WIDTH), 1)
    mark = lax.rem(lane, WIDTH)
    first_of, end_of = jnp.full_like(lane, TILES * span), jnp.zeros_like(lane)
    for d in range(DOCS):
        first_of = jnp.where(mark == d, doc[d], first_of)
        end_of = jnp.where(mark == d, doc[d + 1], end_of)
    low = lane < WIDTH
    key_row = lax.broadcasted_iota(jnp.int32, (keys, 2 * WIDTH), 0)
    kpos[...] = lax.rem(key_row, HALF) + (key_row // HALF) * TOK
    query_row = lax.broadcasted_iota(jnp.int32, (PER * SUB, 2 * WIDTH), 0)
    qpos[...] = lax.rem(query_row, SUB) + (query_row // SUB) * TOK

    def marks(at, same, other):
        return jnp.where((at >= first_of) & (at < end_of), same, other)

    def take_keys(j):
        both = recv_a[pl.ds(j * PER, PER), : 2 * HALF, :]
        k = both[:, :HALF].reshape(keys, 2 * WIDTH)
        one, zero = jnp.float32(1.0), jnp.float32(0.0)
        for half in range(2):
            own = low if half == 0 else jnp.logical_not(low)
            at = kpos[...] + (j * span + half * HALF)
            marked = jnp.where(own, k.astype(jnp.float32), marks(at, one, zero))
            kx[half, j] = marked.astype(jnp.bfloat16)
        v = both[:, HALF:].reshape(keys, 2 * WIDTH)
        v = jnp.transpose(v.astype(jnp.float32), (1, 0)).astype(jnp.bfloat16)
        vt[j, :, :keys] = v[:WIDTH]
        vt[j, :, keys:] = v[WIDTH:]

    def take_queries(i, g):
        if g == 0:
            x = recv_a[pl.ds(i * PER, PER), 2 * HALF :, :]
        else:
            x = recv_b[pl.ds(i * PER, PER)]
        x = x.astype(jnp.float32).reshape(PER * SUB, 2 * WIDTH)
        turned = pltpu.roll(x, WIDTH, 1)
        for late in range(2):
            at = qpos[...] + (i * span + g * SUB + late * HALF)
            m = marks(at, jnp.float32(0.0), jnp.float32(FAR))
            rows = pl.ds(late * PER * SUB, PER * SUB)
            first, second = (x, turned) if late == 0 else (turned, x)
            wq[0, i, rows] = jnp.where(low, first, m).astype(jnp.bfloat16)
            wq[1, i, rows] = jnp.where(low, m, second).astype(jnp.bfloat16)

    def scores_of(i, g, probs):
        spot = lax.broadcasted_iota(jnp.int32, (1, queries), 1)
        within = lax.rem(spot, PER * SUB)
        place = (
            (within // SUB) * TOK + lax.rem(within, SUB) + g * SUB
            + jnp.where(spot >= PER * SUB, HALF, 0)
        )
        total = jnp.zeros((16, queries), jnp.float32)
        for j in range(i + 1):
            for half in range(2):
                p = lax.dot_general(
                    kx[half, j], wq[half, i], (((1,), (1,)), ((), ())),
                    preferred_element_type=jnp.float32,
                )
                p = jnp.exp2(p * SCALE)
                if j == i:
                    at = jnp.concatenate([kpos[...], kpos[...]], axis=1)
                    p = jnp.where(at <= place - half * HALF, p, 0.0)
                probs[j, half * keys : (half + 1) * keys] = p
                total = total + jnp.sum(p.reshape(keys // 16, 16, queries), axis=0)
        return 1.0 / jnp.sum(total, axis=0, keepdims=True)

    def outputs_of(i, g, probs, inverse):
        out = jnp.zeros((WIDTH, queries), jnp.float32)
        for j in range(i + 1):
            weights = (probs[j] * inverse).astype(jnp.bfloat16)
            out = out + jnp.dot(vt[j], weights, preferred_element_type=jnp.float32)
        out = jnp.concatenate([out[:, : PER * SUB], out[:, PER * SUB :]], axis=0)
        out = jnp.transpose(out, (1, 0)).reshape(PER, SUB, 2 * WIDTH)
        back[g, i * PER : (i + 1) * PER] = out.astype(jnp.bfloat16)

    def send_home(i, g, high, c, x):
        p = i * PER + c * NB + x * 2 + high

        @pl.when(p != me)
        def _():
            pltpu.make_async_remote_copy(
                src_ref=back.at[g, p], dst_ref=gathered.at[g, me], send_sem=back_send.at[g],
                recv_sem=back_recv.at[g], device_id={"seqa": 2 * i + c, "seqb": x * 2 + high},
                device_id_type=MESH,
            ).start()

    def pair(first, g):
        second = first + TILES // 2
        small = scores_of(first, g, probs_a)
        large = scores_of(second, g, probs_b)
        outputs_of(first, g, probs_a, small)
        outputs_of(second, g, probs_b, large)
        for c in range(2):
            for x in range(4):
                send_home(first, g, 0, c, x)
                send_home(second, g, 0, c, x)

    def late_half(t, g):
        i = lax.rem(my_tile + jnp.where(lax.rem(t, 2) == 1, TILES - (t + 1) // 2, t // 2), TILES)
        for c in range(2):
            for x in range(4):
                send_home(i, g, 1, c, x)

    def come_in(j, carry):
        arrived(recv_a, ra_sem, j)
        take_keys(j)
        take_queries(j, 0)
        return carry

    def come_in_b(j, carry):
        arrived(recv_b, rb_sem, j)
        take_queries(j, 1)
        return carry

    for g in range(2):
        with jax.named_scope(f"wait_{g}"):
            lax.fori_loop(0, TILES, come_in if g == 0 else come_in_b, 0)

        def step(t, carry):
            m = lax.rem(my_tile, TILES // 2)
            second = jnp.where(m == 0, 1, 0)
            third = jnp.where(m == 0, 2, jnp.where(m == 3, 1, 3))
            i = jnp.where(t == 0, m, jnp.where(t == 1, second, jnp.where(t == 2, third, 6 - m - second - third)))
            lax.switch(i, [functools.partial(pair, k, g) for k in range(TILES // 2)])
            return carry

        with jax.named_scope(f"tiles_{g}"):
            lax.fori_loop(0, TILES // 2, step, 0)

        def rest(t, carry):
            late_half(t, g)
            return carry

        with jax.named_scope(f"rest_{g}"):
            lax.fori_loop(0, TILES, rest, 0)

    for g in range(2):
        gathered[g, me] = back[g, me]
        with jax.named_scope(f"wait_back_{g}"):
            pltpu.make_async_copy(*others(gathered.at[g]), back_recv.at[g]).wait()
        rows_out[...] = gathered[g].astype(jnp.float32).reshape(HEADS * SUB, 2 * WIDTH)
        for r in range(SUB):
            block = jnp.transpose(rows_out[pl.ds(r, HEADS, stride=SUB), :], (1, 0))
            block = block.astype(jnp.bfloat16)
            out_ref[g * SUB + r] = block[:WIDTH]
            out_ref[g * SUB + r + HALF] = block[WIDTH:]
    pltpu.make_async_copy(*others(send_a), send_sem.at[0]).wait()
    pltpu.make_async_copy(*others(send_b), send_sem.at[1]).wait()
    for g in range(2):
        pltpu.make_async_copy(*others(back.at[g]), back_send.at[g]).wait()


def attention(queries, keys, values, doc_bounds, q_gain, k_gain):
    tok, heads, width = queries.shape
    assert (tok, heads, width) == (TOK, HEADS, WIDTH)
    queries, keys, values = (jnp.transpose(a, (0, 2, 1)) for a in (queries, keys, values))
    block = pltpu.VMEM((TOK, WIDTH, HEADS), jnp.bfloat16)
    bf16, f32 = jnp.bfloat16, jnp.float32
    dma = pltpu.SemaphoreType.DMA
    out = pl.pallas_call(
        kernel,
        out_shape=pltpu.VMEM((TOK, WIDTH, HEADS), bf16),
        in_specs=[pl.BlockSpec(memory_space=pl.ANY)] * 6,
        out_specs=pl.BlockSpec(memory_space=pltpu.VMEM),
        scratch_shapes=[
            block, block, block,
            pltpu.SMEM(doc_bounds.shape, jnp.int32),
            pltpu.VMEM((2, 1, WIDTH), f32),
            pltpu.VMEM((HEADS * 3 * HALF, 2 * WIDTH), f32),
            pltpu.VMEM((N, 2 * HALF + SUB, 2 * WIDTH), bf16),
            pltpu.VMEM((N, SUB, 2 * WIDTH), bf16),
            pltpu.VMEM((N, 2 * HALF + SUB, 2 * WIDTH), bf16),
            pltpu.VMEM((N, SUB, 2 * WIDTH), bf16),
            pltpu.VMEM((2, TILES, PER * HALF, 2 * WIDTH), bf16),
            pltpu.VMEM((TILES, WIDTH, 2 * PER * HALF), bf16),
            pltpu.VMEM((TILES // 2, 2 * PER * HALF, 2 * PER * SUB), f32),
            pltpu.VMEM((TILES, 2 * PER * HALF, 2 * PER * SUB), f32),
            pltpu.VMEM((PER * HALF, 2 * WIDTH), jnp.int32),
            pltpu.VMEM((PER * SUB, 2 * WIDTH), jnp.int32),
            pltpu.VMEM((2, TILES, 2 * PER * SUB, 2 * WIDTH), bf16),
            pltpu.VMEM((2, N, SUB, 2 * WIDTH), bf16),
            pltpu.VMEM((2, N, SUB, 2 * WIDTH), bf16),
            pltpu.VMEM((HEADS * SUB, 2 * WIDTH), f32),
            dma((6,)), dma((2,)), dma((TILES,)), dma((TILES,)), dma((2,)), dma((2,)),
            pltpu.SemaphoreType.REGULAR((9,)), pltpu.SemaphoreType.REGULAR((8,)),
        ],
        compiler_params=pltpu.CompilerParams(
            collective_id=0, has_side_effects=True, vmem_limit_bytes=60 << 20
        ),
    )(queries, keys, values, doc_bounds, q_gain.reshape(1, WIDTH), k_gain.reshape(1, WIDTH))
    return jnp.transpose(out, (0, 2, 1))


def solution(mesh):
    assert mesh.shape["seqa"] * mesh.shape["seqb"] == N and mesh.shape["seqb"] == NB
    rows = P(("dp", "seqa", "seqb"), None, None)
    return jax.shard_map(
        attention,
        mesh=mesh,
        in_specs=(rows, rows, rows, P("dp"), P(), P()),
        out_specs=rows,
        check_vma=False,
    )
```

```python
import functools
import math

import jax
import jax.numpy as jnp
import numpy as np
from jax import lax
from jax.experimental import pallas as pl
from jax.experimental.pallas import tpu as pltpu
from jax.sharding import PartitionSpec as P

MESH = pl.DeviceIdType.MESH
DOCS = 8
TOK, HEADS, WIDTH = 32, 128, 64
N, NB = 128, 8
HALF = TOK // 2
SUB = HALF // 2
TILES = 8
PER = N // TILES
FAR = -2048.0
SCALE = math.log2(math.e) / math.sqrt(WIDTH)
LOG_BASE = np.float32(-np.log(np.float32(10000.0)))
FREQS = [
    float(np.float32(np.exp(np.float64(np.float32(LOG_BASE * np.float32(i)) * 2.0 / WIDTH))))
    for i in range(WIDTH // 2)
]


def cos_sin(angle):
    turns = jnp.floor(angle * 0.6366197723675814 + 0.5)
    r = angle - turns * 1.5703125
    r = r - turns * 4.837512969970703125e-4
    r = r - turns * 7.54978995489188216e-8
    z = r * r
    s = ((-1.9515295891e-4 * z + 8.3321608736e-3) * z - 1.6666654611e-1) * z * r + r
    c = ((2.443315711809948e-5 * z - 1.388731625493765e-3) * z + 4.166664568298827e-2) * z * z
    c = c - 0.5 * z + 1.0
    quarter = turns.astype(jnp.int32)
    odd = (quarter & 1) == 1
    cosine = jnp.where(odd, s, c)
    sine = jnp.where(odd, c, s)
    cosine = jnp.where(((quarter + 1) & 2) == 2, -cosine, cosine)
    sine = jnp.where((quarter & 2) == 2, -sine, sine)
    return cosine, sine


def start_of(place, doc):
    start = jnp.zeros_like(place)
    for d in range(1, DOCS):
        start = jnp.where(place >= doc[d], doc[d], start)
    return start


def kernel(
    q_hbm, k_hbm, v_hbm, doc_hbm, qg_hbm, kg_hbm, out_ref,
    qb, kb, vb, doc, gains, stage, send_a, send_b, recv_a, recv_b, kx, vt, probs_a, probs_b, kpos, qpos,
    wq,    back, gathered, rows_out,
    in_sem, send_sem, ra_sem, rb_sem, back_send, back_recv, from_below, from_above,
):
    seqa, seqb = lax.axis_index("seqa"), lax.axis_index("seqb")
    me = seqa * NB + seqb
    my_tile = seqa // 2
    core, chip_x, chip_z = lax.rem(seqa, 2), seqb // 2, lax.rem(seqb, 2) * 8 + my_tile
    across = [(chip_x, core)] + [
        (lax.rem(chip_x + i // 2, 4), lax.rem(core + i, 2)) for i in range(1, 8)
    ]

    def at_plane(z):
        z = lax.rem(z, 16)
        low, high = lax.rem(z, 8), z // 8
        return [
            (low * 16 + c * 8 + x * 2 + high, {"seqa": low * 2 + c, "seqb": x * 2 + high})
            for x, c in across
        ]

    with jax.named_scope("greet"):
        loads = [
            pltpu.make_async_copy(src, dst, in_sem.at[i])
            for i, (src, dst) in enumerate(
                (
                    (doc_hbm, doc), (qg_hbm, gains.at[0]), (kg_hbm, gains.at[1]),
                    (q_hbm, qb), (k_hbm, kb), (v_hbm, vb),
                )
            )
        ]
        for load in loads:
            load.start()
        barrier = pltpu.get_barrier_semaphore()
        above, below = at_plane(chip_z + 1)[0][1], at_plane(chip_z + 15)[0][1]
        for where in [at[1] for at in at_plane(chip_z)[1:]] + [above, below]:
            pl.semaphore_signal(barrier, inc=1, device_id=where, device_id_type=MESH)

    row = lax.broadcasted_iota(jnp.int32, (WIDTH // 2, HEADS), 0)
    freq = jnp.zeros((WIDTH // 2, HEADS), jnp.float32)
    for i, f in enumerate(FREQS):
        freq = jnp.where(row == i, jnp.float32(f), freq)
    with jax.named_scope("load"):
        for load in loads:
            load.wait()
    gq, gk = (
        jnp.transpose(jnp.broadcast_to(gains[i], (HEADS, WIDTH)), (1, 0)) for i in range(2)
    )
    place = me * TOK + lax.broadcasted_iota(jnp.int32, (1, HEADS), 1)
    cosines, sines = cos_sin((place - start_of(place, doc)).astype(jnp.float32) * freq)

    def prepared(x, gain, cosine, sine):
        x = x.astype(jnp.float32)
        mean = jnp.sum(x * x, axis=0, keepdims=True) * (1.0 / WIDTH)
        x = x * lax.rsqrt(mean + 1e-06) * gain
        a, b = x[: WIDTH // 2], x[WIDTH // 2 :]
        return a * cosine - b * sine, a * sine + b * cosine

    with jax.named_scope("prep"):
        for r in range(HALF):
            parts_q, parts_k, parts_v = [], [], []
            for t in (r, r + HALF):
                cosine, sine = (
                    jnp.broadcast_to(table[:, t : t + 1], (WIDTH // 2, HEADS))
                    for table in (cosines, sines)
                )
                parts_q.extend(prepared(qb[t], gq, cosine, sine))
                parts_k.extend(prepared(kb[t], gk, cosine, sine))
                parts_v.append(vb[t].astype(jnp.float32))
            for at, parts in ((0, parts_k), (HALF, parts_v), (2 * HALF, parts_q)):
                block = jnp.transpose(jnp.concatenate(parts, axis=0), (1, 0))
                stage[pl.ds(at + r, HEADS, stride=3 * HALF), :] = block

    def pack(h, carry):
        rows = stage[pl.ds(pl.multiple_of(h * 8 * 3 * HALF, 8), 8 * 3 * HALF), :]
        rows = rows.reshape(8, 3 * HALF, 2 * WIDTH)
        send_a[pl.ds(h * 8, 8)] = rows[:, : 2 * HALF + SUB].astype(jnp.bfloat16)
        send_b[pl.ds(h * 8, 8)] = rows[:, 2 * HALF + SUB :].astype(jnp.bfloat16)
        return carry

    with jax.named_scope("pack"):
        lax.fori_loop(0, HEADS // 8, pack, 0)

    def post(which, p, where):
        source, target, arrival = (
            (send_a, recv_a, ra_sem), (send_b, recv_b, rb_sem)
        )[which]
        pltpu.make_async_remote_copy(
            src_ref=source.at[p], dst_ref=target.at[me], send_sem=send_sem.at[which],
            recv_sem=arrival.at[my_tile], device_id=where, device_id_type=MESH,
        ).start()

    def post_mixed(which, spots):
        for i in spots:
            x, c = across[i]

            def one(k, carry):
                away = jnp.where(lax.rem(k, 2) == 1, 8 - (k + 1) // 2, 8 + k // 2)
                z = lax.rem(chip_z + away, 16)
                low, high = lax.rem(z, 8), z // 8
                post(
                    which, low * 16 + c * 8 + x * 2 + high,
                    {"seqa": low * 2 + c, "seqb": x * 2 + high},
                )
                return carry

            lax.fori_loop(0, 15 if i == 0 else 16, one, 0)

    def tell(sem, where):
        pl.semaphore_signal(sem, inc=1, device_id=where, device_id_type=MESH)

    with jax.named_scope("barrier"):
        pl.semaphore_wait(barrier, 9)
    near = 4
    with jax.named_scope("post_a"):
        tell(from_below.at[1], above)
        tell(from_above.at[1], below)
        for at in at_plane(chip_z)[1:near]:
            post(0, *at)

        def ring(k, carry):
            pl.semaphore_wait(from_below.at[k], 1)
            tell(from_below.at[k + 1], above)
            pl.semaphore_wait(from_above.at[k], 1)

            @pl.when(k < 7)
            def _():
                tell(from_above.at[k + 1], below)

            for at in at_plane(chip_z + 16 - k)[:near] + at_plane(chip_z + k)[:near]:
                post(0, *at)
            return carry

        lax.fori_loop(1, 8, ring, 0)
        pl.semaphore_wait(from_below.at[8], 1)
        for at in at_plane(chip_z + 8)[:near]:
            post(0, *at)
        post_mixed(0, range(near, 8))
    with jax.named_scope("post_b"):
        post_mixed(1, range(8))
    own_a = pltpu.make_async_copy(send_a.at[me], recv_a.at[me], ra_sem.at[my_tile])
    own_b = pltpu.make_async_copy(send_b.at[me], recv_b.at[me], rb_sem.at[my_tile])
    own_a.start()
    own_b.start()

    def others(ref):
        part = ref.at[pl.ds(1, N - 1)]
        return part, part

    def arrived(ref, sem, j):
        part = ref.at[pl.ds(pl.multiple_of(j * PER, PER), PER)]
        pltpu.make_async_copy(part, part, sem.at[j]).wait()

    queries, span, keys = 2 * PER * SUB, PER * TOK, PER * HALF
    lane = lax.broadcasted_iota(jnp.int32, (1, 2 * WIDTH), 1)
    mark = lax.rem(lane, WIDTH)
    first_of, end_of = jnp.full_like(lane, TILES * span), jnp.zeros_like(lane)
    for d in range(DOCS):
        first_of = jnp.where(mark == d, doc[d], first_of)
        end_of = jnp.where(mark == d, doc[d + 1], end_of)
    low = lane < WIDTH
    key_row = lax.broadcasted_iota(jnp.int32, (keys, 2 * WIDTH), 0)
    kpos[...] = lax.rem(key_row, HALF) + (key_row // HALF) * TOK
    query_row = lax.broadcasted_iota(jnp.int32, (PER * SUB, 2 * WIDTH), 0)
    qpos[...] = lax.rem(query_row, SUB) + (query_row // SUB) * TOK

    def marks(at, same, other):
        return jnp.where((at >= first_of) & (at < end_of), same, other)

    def take_keys(j):
        both = recv_a[pl.ds(j * PER, PER), : 2 * HALF, :]
        k = both[:, :HALF].reshape(keys, 2 * WIDTH)
        one, zero = jnp.float32(1.0), jnp.float32(0.0)
        for half in range(2):
            own = low if half == 0 else jnp.logical_not(low)
            at = kpos[...] + (j * span + half * HALF)
            marked = jnp.where(own, k.astype(jnp.float32), marks(at, one, zero))
            kx[half, j] = marked.astype(jnp.bfloat16)
        v = both[:, HALF:].reshape(keys, 2 * WIDTH)
        v = jnp.transpose(v.astype(jnp.float32), (1, 0)).astype(jnp.bfloat16)
        vt[j, :, :keys] = v[:WIDTH]
        vt[j, :, keys:] = v[WIDTH:]

    def take_queries(i, g):
        if g == 0:
            x = recv_a[pl.ds(i * PER, PER), 2 * HALF :, :]
        else:
            x = recv_b[pl.ds(i * PER, PER)]
        x = x.astype(jnp.float32).reshape(PER * SUB, 2 * WIDTH)
        turned = pltpu.roll(x, WIDTH, 1)
        for late in range(2):
            at = qpos[...] + (i * span + g * SUB + late * HALF)
            m = marks(at, jnp.float32(0.0), jnp.float32(FAR))
            rows = pl.ds(late * PER * SUB, PER * SUB)
            first, second = (x, turned) if late == 0 else (turned, x)
            wq[0, i, rows] = jnp.where(low, first, m).astype(jnp.bfloat16)
            wq[1, i, rows] = jnp.where(low, m, second).astype(jnp.bfloat16)

    def scores_of(i, g, probs):
        spot = lax.broadcasted_iota(jnp.int32, (1, queries), 1)
        within = lax.rem(spot, PER * SUB)
        place = (
            (within // SUB) * TOK + lax.rem(within, SUB) + g * SUB
            + jnp.where(spot >= PER * SUB, HALF, 0)
        )
        total = jnp.zeros((16, queries), jnp.float32)
        for j in range(i + 1):
            for half in range(2):
                p = lax.dot_general(
                    kx[half, j], wq[half, i], (((1,), (1,)), ((), ())),
                    preferred_element_type=jnp.float32,
                )
                p = jnp.exp2(p * SCALE)
                if j == i:
                    at = jnp.concatenate([kpos[...], kpos[...]], axis=1)
                    p = jnp.where(at <= place - half * HALF, p, 0.0)
                probs[j, half * keys : (half + 1) * keys] = p
                total = total + jnp.sum(p.reshape(keys // 16, 16, queries), axis=0)
        return 1.0 / jnp.sum(total, axis=0, keepdims=True)

    def outputs_of(i, g, probs, inverse):
        out = jnp.zeros((WIDTH, queries), jnp.float32)
        for j in range(i + 1):
            weights = (probs[j] * inverse).astype(jnp.bfloat16)
            out = out + jnp.dot(vt[j], weights, preferred_element_type=jnp.float32)
        out = jnp.concatenate([out[:, : PER * SUB], out[:, PER * SUB :]], axis=0)
        out = jnp.transpose(out, (1, 0)).reshape(PER, SUB, 2 * WIDTH)
        back[g, i * PER : (i + 1) * PER] = out.astype(jnp.bfloat16)

    def send_home(i, g, high, c, x):
        p = i * PER + c * NB + x * 2 + high

        @pl.when(p != me)
        def _():
            pltpu.make_async_remote_copy(
                src_ref=back.at[g, p], dst_ref=gathered.at[g, me], send_sem=back_send.at[g],
                recv_sem=back_recv.at[g], device_id={"seqa": 2 * i + c, "seqb": x * 2 + high},
                device_id_type=MESH,
            ).start()

    def pair(first, g):
        second = first + TILES // 2
        small = scores_of(first, g, probs_a)
        large = scores_of(second, g, probs_b)
        outputs_of(first, g, probs_a, small)
        outputs_of(second, g, probs_b, large)
        for c in (1, 0):
            for x in range(4):
                send_home(first, g, 0, c, x)
                send_home(second, g, 0, c, x)

    def late_half(t, g):
        i = lax.rem(my_tile + jnp.where(lax.rem(t, 2) == 1, TILES - (t + 1) // 2, t // 2), TILES)
        for c in range(2):
            for x in range(4):
                send_home(i, g, 1, c, x)

    def come_in(j, carry):
        arrived(recv_a, ra_sem, j)
        take_keys(j)
        take_queries(j, 0)
        return carry

    def come_in_b(j, carry):
        arrived(recv_b, rb_sem, j)
        take_queries(j, 1)
        return carry

    for g in range(2):
        with jax.named_scope(f"wait_{g}"):
            lax.fori_loop(0, TILES, come_in if g == 0 else come_in_b, 0)

        def step(t, carry):
            m = lax.rem(my_tile, TILES // 2)
            second = jnp.where(m == 0, 1, 0)
            third = jnp.where(m == 0, 2, jnp.where(m == 3, 1, 3))
            i = jnp.where(t == 0, m, jnp.where(t == 1, second, jnp.where(t == 2, third, 6 - m - second - third)))
            lax.switch(i, [functools.partial(pair, k, g) for k in range(TILES // 2)])
            return carry

        with jax.named_scope(f"tiles_{g}"):
            lax.fori_loop(0, TILES // 2, step, 0)

        def rest(t, carry):
            late_half(t, g)
            return carry

        with jax.named_scope(f"rest_{g}"):
            lax.fori_loop(0, TILES, rest, 0)

    for g in range(2):
        gathered[g, me] = back[g, me]
        with jax.named_scope(f"wait_back_{g}"):
            pltpu.make_async_copy(*others(gathered.at[g]), back_recv.at[g]).wait()
        rows_out[...] = gathered[g].astype(jnp.float32).reshape(HEADS * SUB, 2 * WIDTH)
        for r in range(SUB):
            block = jnp.transpose(rows_out[pl.ds(r, HEADS, stride=SUB), :], (1, 0))
            block = block.astype(jnp.bfloat16)
            out_ref[g * SUB + r] = block[:WIDTH]
            out_ref[g * SUB + r + HALF] = block[WIDTH:]
    pltpu.make_async_copy(*others(send_a), send_sem.at[0]).wait()
    pltpu.make_async_copy(*others(send_b), send_sem.at[1]).wait()
    for g in range(2):
        pltpu.make_async_copy(*others(back.at[g]), back_send.at[g]).wait()


def attention(queries, keys, values, doc_bounds, q_gain, k_gain):
    tok, heads, width = queries.shape
    assert (tok, heads, width) == (TOK, HEADS, WIDTH)
    queries, keys, values = (jnp.transpose(a, (0, 2, 1)) for a in (queries, keys, values))
    block = pltpu.VMEM((TOK, WIDTH, HEADS), jnp.bfloat16)
    bf16, f32 = jnp.bfloat16, jnp.float32
    dma = pltpu.SemaphoreType.DMA
    out = pl.pallas_call(
        kernel,
        out_shape=pltpu.VMEM((TOK, WIDTH, HEADS), bf16),
        in_specs=[pl.BlockSpec(memory_space=pl.ANY)] * 6,
        out_specs=pl.BlockSpec(memory_space=pltpu.VMEM),
        scratch_shapes=[
            block, block, block,
            pltpu.SMEM(doc_bounds.shape, jnp.int32),
            pltpu.VMEM((2, 1, WIDTH), f32),
            pltpu.VMEM((HEADS * 3 * HALF, 2 * WIDTH), f32),
            pltpu.VMEM((N, 2 * HALF + SUB, 2 * WIDTH), bf16),
            pltpu.VMEM((N, SUB, 2 * WIDTH), bf16),
            pltpu.VMEM((N, 2 * HALF + SUB, 2 * WIDTH), bf16),
            pltpu.VMEM((N, SUB, 2 * WIDTH), bf16),
            pltpu.VMEM((2, TILES, PER * HALF, 2 * WIDTH), bf16),
            pltpu.VMEM((TILES, WIDTH, 2 * PER * HALF), bf16),
            pltpu.VMEM((TILES // 2, 2 * PER * HALF, 2 * PER * SUB), f32),
            pltpu.VMEM((TILES, 2 * PER * HALF, 2 * PER * SUB), f32),
            pltpu.VMEM((PER * HALF, 2 * WIDTH), jnp.int32),
            pltpu.VMEM((PER * SUB, 2 * WIDTH), jnp.int32),
            pltpu.VMEM((2, TILES, 2 * PER * SUB, 2 * WIDTH), bf16),
            pltpu.VMEM((2, N, SUB, 2 * WIDTH), bf16),
            pltpu.VMEM((2, N, SUB, 2 * WIDTH), bf16),
            pltpu.VMEM((HEADS * SUB, 2 * WIDTH), f32),
            dma((6,)), dma((2,)), dma((TILES,)), dma((TILES,)), dma((2,)), dma((2,)),
            pltpu.SemaphoreType.REGULAR((9,)), pltpu.SemaphoreType.REGULAR((8,)),
        ],
        compiler_params=pltpu.CompilerParams(
            collective_id=0, has_side_effects=True, vmem_limit_bytes=60 << 20
        ),
    )(queries, keys, values, doc_bounds, q_gain.reshape(1, WIDTH), k_gain.reshape(1, WIDTH))
    return jnp.transpose(out, (0, 2, 1))


def solution(mesh):
    assert mesh.shape["seqa"] * mesh.shape["seqb"] == N and mesh.shape["seqb"] == NB
    rows = P(("dp", "seqa", "seqb"), None, None)
    return jax.shard_map(
        attention,
        mesh=mesh,
        in_specs=(rows, rows, rows, P("dp"), P(), P()),
        out_specs=rows,
        check_vma=False,
    )
```
